32 devices in a mesh: batch: 8 (over z, y), space: 4 (over x, core).
Axes of the slice: x: 2, y: 2, z: 4, core: 2. Of those that a mesh axis runs over, the one named last changes fastest.
Arguments:
- features: bfloat16 [8, 48, 72, 1024], P('batch', 'space'), may hold values from -600 to 600
- depth_one: bfloat16 [3, 3, 1024], replicated, may hold values from -2 to 2
- gain_one: float32 [1024], replicated, may hold values from 0.25 to 1.75
- shift_one: float32 [1024], replicated, may hold values from -3 to 3
- point_one: bfloat16 [1024, 1536], replicated, may hold values from -0.1875 to 0.1875
- gain_two: float32 [1536], replicated, may hold values from 0.25 to 1.75
- shift_two: float32 [1536], replicated, may hold values from -3 to 3
- depth_two: bfloat16 [3, 3, 1536], replicated, may hold values from -2 to 2
- gain_three: float32 [1536], replicated, may hold values from 0.25 to 1.75
- shift_three: float32 [1536], replicated, may hold values from -3 to 3
- point_two: bfloat16 [1536, 2048], replicated, may hold values from -0.15625 to 0.15625
- gain_four: float32 [2048], replicated, may hold values from 0.25 to 1.75
- shift_four: float32 [2048], replicated, may hold values from -3 to 3
Outputs:
- exit_map: bfloat16 [8, 48, 72, 2048], P('batch', 'space')
The draws below stay inside these ranges and needn't reach their ends.
All inputs are finite; a program needn't handle non-finite values.
Results may differ from the reference program's by a relative error of at most 0.0079.
Values may be sent and summed in bfloat16 or wider, within the bound.
A program may use at most 64 MiB of HBM per device.

```python
import jax
import jax.numpy as jnp
from jax import lax

CH_IN = 1024
CH_MID = 1536
CH_OUT = 2048
COLS = 72
RATE = 2
LATS = 48
SAMPLES = 8


def draw_features(key, part):
    key_base, key_chan = jax.random.split(key, 2)
    sample_ramp = 3.0 ** (jnp.arange(SAMPLES, dtype=jnp.float32) / max(SAMPLES - 1, 1))
    row_ramp = 3.0 ** (jnp.arange(LATS, dtype=jnp.float32) / max(LATS - 1, 1))
    base = jnp.clip(jax.random.normal(key_base, (SAMPLES, LATS, COLS, CH_IN), jnp.float32), -6.0, 6.0)
    channel_scale = jax.random.uniform(key_chan, (CH_IN,), jnp.float32, 0.5, 2.0)
    values = base * sample_ramp[:, None, None, None] * row_ramp[None, :, None, None] * channel_scale
    return values.astype(jnp.bfloat16)


def bell_draw(stream_key, shape, deviation, limit, kind=jnp.bfloat16):
    entries = jax.random.normal(stream_key, shape, jnp.float32) * deviation
    return jnp.minimum(jnp.maximum(entries, -limit), limit).astype(kind)


def setup_inputs(seed: int = 0) -> dict:
    seeds = jax.random.split(jax.random.key(seed), 14)
    features = draw_features(jax.random.fold_in(seeds[13], 71), 0)
    depth_one = bell_draw(seeds[1], (3, 3, CH_IN), 9 ** -0.5, 2.0)
    gain_one = jnp.clip(1.0 + 0.15 * jax.random.normal(seeds[2], (CH_IN,), jnp.float32), 0.25, 1.75)
    shift_one = bell_draw(seeds[3], (CH_IN,), 0.5, 3.0, jnp.float32)
    point_one = bell_draw(seeds[4], (CH_IN, CH_MID), CH_IN ** -0.5, 0.1875)
    gain_two = jnp.clip(1.0 + 0.15 * jax.random.normal(seeds[5], (CH_MID,), jnp.float32), 0.25, 1.75)
    shift_two = bell_draw(seeds[6], (CH_MID,), 0.5, 3.0, jnp.float32)
    depth_two = bell_draw(seeds[7], (3, 3, CH_MID), 9 ** -0.5, 2.0)
    gain_three = jnp.clip(1.0 + 0.15 * jax.random.normal(seeds[8], (CH_MID,), jnp.float32), 0.25, 1.75)
    shift_three = bell_draw(seeds[9], (CH_MID,), 0.5, 3.0, jnp.float32)
    point_two = bell_draw(seeds[10], (CH_MID, CH_OUT), CH_MID ** -0.5, 0.15625)
    gain_four = jnp.clip(1.0 + 0.15 * jax.random.normal(seeds[11], (CH_OUT,), jnp.float32), 0.25, 1.75)
    shift_four = bell_draw(seeds[12], (CH_OUT,), 0.5, 3.0, jnp.float32)
    return {"features": features, "depth_one": depth_one, "gain_one": gain_one, "shift_one": shift_one, "point_one": point_one, "gain_two": gain_two, "shift_two": shift_two, "depth_two": depth_two, "gain_three": gain_three, "shift_three": shift_three, "point_two": point_two, "gain_four": gain_four, "shift_four": shift_four}


epsilon = 1e-05

def dilated(values, weight):
    span_rows = values.shape[1]
    span_cols = values.shape[2]
    padded = jnp.pad(values, ((0, 0), (RATE, RATE), (RATE, RATE), (0, 0)))
    summed = jnp.zeros(values.shape, jnp.float32)
    for tap_row in range(3):
        for tap_col in range(3):
            window = padded[:, tap_row * RATE:tap_row * RATE + span_rows, tap_col * RATE:tap_col * RATE + span_cols, :]
            summed = summed + window.astype(jnp.float32) * weight[tap_row, tap_col].astype(jnp.float32)
    return summed

def normalize(values, gain, offset):
    pixels = values.shape[0] * values.shape[1] * values.shape[2]
    average = lax.optimization_barrier(jnp.sum(values, axis=(0, 1, 2))) / pixels
    variance = lax.optimization_barrier(jnp.sum(values * values, axis=(0, 1, 2))) / pixels - average * average
    factor = gain * lax.rsqrt(variance + epsilon)
    return jnp.maximum((values - average) * factor + offset, 0.0).astype(jnp.bfloat16)

def project(values, weight):
    shape = values.shape
    flat = values.reshape(shape[0] * shape[1] * shape[2], shape[3])
    result = jnp.dot(flat, weight, preferred_element_type=jnp.float32)
    return result.reshape(shape[0], shape[1], shape[2], weight.shape[1])

def reference(features, depth_one, gain_one, shift_one, point_one, gain_two, shift_two, depth_two, gain_three, shift_three, point_two, gain_four, shift_four):
    act_one = normalize(dilated(features, depth_one), gain_one, shift_one)
    act_two = normalize(project(act_one, point_one), gain_two, shift_two)
    act_three = normalize(dilated(act_two, depth_two), gain_three, shift_three)
    return normalize(project(act_three, point_two), gain_four, shift_four)
```

```python
import functools

import jax
import jax.numpy as jnp
from jax import lax
from jax.experimental import pallas as pl
from jax.experimental.pallas import tpu as pltpu
from jax.sharding import PartitionSpec as P

RATE = 2
PIECES = 4
EPS = 1e-05
LANES = 128
PAD = 8
NCOL = 256
MESH = pl.DeviceIdType.MESH
F32 = jnp.float32
BF16 = jnp.bfloat16


def block_rows(pixels):
    for rows in (144, 96, 48, 32, 16):
        if pixels % rows == 0:
            return rows
    return pixels


def kernel(
    n_space,
    n_batch,
    x_hbm,
    w1_hbm,
    w2_hbm,
    d1_ref,
    d2_ref,
    g1_ref,
    b1_ref,
    g2_ref,
    b2_ref,
    g3_ref,
    b3_ref,
    g4_ref,
    b4_ref,
    fourth,
    mean_out,
    fac_out,
    shift_out,
    x_ref,
    w1_ref,
    w2_ref,
    halo1,
    edge2,
    halo2,
    xp,
    first,
    act1,
    second,
    act3,
    par_ref,
    sa0,
    sa1,
    sa2,
    sa3,
    sb0,
    sb1,
    sb2,
    sb3,
    coef,
    load_sem,
    h1_send,
    h1_recv,
    h2_send,
    h2_recv,
    a_send,
    a_recv,
    b_send,
    b_recv,
):
    rows, cols, c_in = x_hbm.shape
    c_mid = w1_hbm.shape[1]
    c_out = w2_hbm.shape[1]
    pixels = rows * cols
    edge = RATE * cols
    total = float(pixels * n_space * n_batch)
    step = block_rows(pixels)
    n_in, n_mid, n_out = c_in // LANES, c_mid // LANES, c_out // LANES
    sp = lax.axis_index("space")
    bt = lax.axis_index("batch")
    has_top = sp > 0
    has_bot = sp < n_space - 1
    sa = (sa0, sa1, sa2, sa3)
    sb = (sb0, sb1, sb2, sb3)

    load_x = pltpu.make_async_copy(x_hbm, x_ref, load_sem.at[0])
    load_w1 = pltpu.make_async_copy(w1_hbm, w1_ref, load_sem.at[1])
    load_w2 = pltpu.make_async_copy(w2_hbm, w2_ref, load_sem.at[2])

    barrier = pltpu.get_barrier_semaphore()
    for d in range(1, n_space):
        pl.semaphore_signal(
            barrier, inc=1, device_id={"space": lax.rem(sp + d, n_space)}, device_id_type=MESH
        )
    for d in range(1, n_batch):
        pl.semaphore_signal(
            barrier, inc=1, device_id={"batch": lax.rem(bt + d, n_batch)}, device_id_type=MESH
        )
    load_x.start()
    load_w1.start()
    load_w2.start()

    def clear(j, carry):
        for r in range(rows + 2 * RATE):
            xp[j, r, 0:PAD, :] = jnp.zeros((PAD, LANES), F32)
            xp[j, r, PAD + cols : PAD + cols + PAD, :] = jnp.zeros((PAD, LANES), F32)
        return carry

    lax.fori_loop(0, c_mid // LANES, clear, 0)
    at = 0
    for ref in (g1_ref, b1_ref, g2_ref, b2_ref, g3_ref, b3_ref, g4_ref, b4_ref):
        for j in range(ref.shape[0] // LANES):
            par_ref[at : at + 1, :] = ref[j * LANES : (j + 1) * LANES].reshape(1, LANES)
            at += 1
    load_x.wait()
    pl.semaphore_wait(barrier, n_space - 1 + n_batch - 1)

    wide_in = c_in // PIECES

    def up1(p):
        lanes = pl.ds(p * wide_in, wide_in)
        return pltpu.make_async_remote_copy(
            src_ref=x_ref.at[pl.ds(rows - RATE, RATE), :, lanes],
            dst_ref=halo1.at[0, :, :, lanes],
            send_sem=h1_send.at[0, p],
            recv_sem=h1_recv.at[0, p],
            device_id={"space": sp + 1},
            device_id_type=MESH,
        )

    def down1(p):
        lanes = pl.ds(p * wide_in, wide_in)
        return pltpu.make_async_remote_copy(
            src_ref=x_ref.at[pl.ds(0, RATE), :, lanes],
            dst_ref=halo1.at[1, :, :, lanes],
            send_sem=h1_send.at[1, p],
            recv_sem=h1_recv.at[1, p],
            device_id={"space": sp - 1},
            device_id_type=MESH,
        )

    for p in range(PIECES):

        @pl.when(has_bot)
        def _():
            up1(p).start()

        @pl.when(has_top)
        def _():
            down1(p).start()

    @pl.when(jnp.logical_not(has_top))
    def _():
        halo1[0] = jnp.zeros(halo1.shape[1:], BF16)

    @pl.when(jnp.logical_not(has_bot))
    def _():
        halo1[1] = jnp.zeros(halo1.shape[1:], BF16)

    def taps(d_ref, lanes):
        return [
            [d_ref[a, b : b + 1, lanes].astype(F32) for b in range(3)] for a in range(3)
        ]

    def conv_row(j, r, filt):
        acc = None
        for a in range(3):
            for b in range(3):
                term = xp[j, r + RATE * a, pl.ds(PAD + RATE * (b - 1), cols), :] * filt[a][b]
                acc = term if acc is None else acc + term
        return acc

    def lanes_of(j):
        return pl.ds(pl.multiple_of(j * LANES, LANES), LANES)

    def fold(v):
        s = v[0:8]
        for k in range(1, v.shape[0] // 8):
            s = s + v[8 * k : 8 * k + 8]
        return s

    def conv_rows(j, row_list, d_ref, dst, s1, s2):
        lanes = lanes_of(j)
        filt = taps(d_ref, lanes)
        for r in row_list:
            y = conv_row(j, r, filt)
            dst[r * cols : (r + 1) * cols, lanes] = y
            s1 = s1 + fold(y)
            s2 = s2 + fold(y * y)
        return s1, s2

    def put_stats(buf, slot, row, count, s1, s2):
        buf[slot, pl.ds(row, 1), :] = jnp.sum(s1, axis=0, keepdims=True)
        buf[slot, pl.ds(row + count, 1), :] = jnp.sum(s2, axis=0, keepdims=True)

    def exchange_a(i, d):
        return pltpu.make_async_remote_copy(
            src_ref=sa[i].at[sp],
            dst_ref=sa[i].at[sp],
            send_sem=a_send.at[i, d - 1],
            recv_sem=a_recv.at[i, d - 1],
            device_id={"space": lax.rem(sp + d, n_space)},
            device_id_type=MESH,
        )

    def exchange_b(i, d):
        return pltpu.make_async_remote_copy(
            src_ref=sb[i].at[bt],
            dst_ref=sb[i].at[bt],
            send_sem=b_send.at[i, d - 1],
            recv_sem=b_recv.at[i, d - 1],
            device_id={"batch": lax.rem(bt + d, n_batch)},
            device_id_type=MESH,
        )

    def reduce_stats(i, count, at, between=lambda: None):
        for d in range(1, n_space):
            exchange_a(i, d).start()
        between()
        for d in range(1, n_space):
            exchange_a(i, d).wait_recv()
        s = sa[i][0]
        for k in range(1, n_space):
            s = s + sa[i][k]
        sb[i][bt] = s
        for d in range(1, n_batch):
            exchange_b(i, d).start()
        for d in range(1, n_batch):
            exchange_b(i, d).wait_recv()
        s = sb[i][0]
        for k in range(1, n_batch):
            s = s + sb[i][k]
        mean = s[:count] / total
        var = s[count:] / total - mean * mean
        fac = par_ref[at : at + count] * lax.rsqrt(var + EPS)
        coef[0, 0:count] = mean
        coef[1, 0:count] = fac
        coef[2, 0:count] = par_ref[at + count : at + 2 * count]
        for d in range(1, n_space):
            exchange_a(i, d).wait_send()
        for d in range(1, n_batch):
            exchange_b(i, d).wait_send()

    def normal(v, j):
        return jnp.maximum(
            (v - coef[0, pl.ds(j, 1), :]) * coef[1, pl.ds(j, 1), :] + coef[2, pl.ds(j, 1), :], 0.0
        ).astype(BF16)

    zero8 = jnp.zeros((8, LANES), F32)
    inner = list(range(RATE, rows - RATE))
    outer = list(range(RATE)) + list(range(rows - RATE, rows))


    def conv1_inner(j, carry):
        lanes = lanes_of(j)
        for r in range(rows):
            xp[j, r + RATE, PAD : PAD + cols, :] = x_ref[r, :, lanes].astype(F32)
        s1, s2 = conv_rows(j, inner, d1_ref, first, zero8, zero8)
        coef[3, pl.ds(pl.multiple_of(j * 8, 8), 8), :] = s1
        coef[4, pl.ds(pl.multiple_of(j * 8, 8), 8), :] = s2
        return carry

    lax.fori_loop(0, n_in, conv1_inner, 0)

    def conv1_outer(j, carry):
        lanes = lanes_of(j)
        for r in range(RATE):
            xp[j, r, PAD : PAD + cols, :] = halo1[0, r, :, lanes].astype(F32)
            xp[j, rows + RATE + r, PAD : PAD + cols, :] = halo1[1, r, :, lanes].astype(F32)
        s1 = coef[3, pl.ds(pl.multiple_of(j * 8, 8), 8), :]
        s2 = coef[4, pl.ds(pl.multiple_of(j * 8, 8), 8), :]
        s1, s2 = conv_rows(j, outer, d1_ref, first, s1, s2)
        put_stats(sa0, sp, j, n_in, s1, s2)
        return carry

    for p in range(PIECES):

        @pl.when(has_top)
        def _():
            up1(p).wait_recv()

        @pl.when(has_bot)
        def _():
            down1(p).wait_recv()

        lax.fori_loop(p * n_in // PIECES, (p + 1) * n_in // PIECES, conv1_outer, 0)
    reduce_stats(0, n_in, 0)

    for p in range(PIECES):

        @pl.when(has_bot)
        def _():
            up1(p).wait_send()

        @pl.when(has_top)
        def _():
            down1(p).wait_send()

    def norm_to(src, dst, count):
        def body(j, carry):
            lanes = lanes_of(j)
            for k in range(pixels // step):
                span = slice(k * step, (k + 1) * step)
                dst[span, lanes] = normal(src[span, lanes], j)
            return carry

        lax.fori_loop(0, count, body, 0)

    norm_to(first, act1, n_in)

    def up2(n):
        return pltpu.make_async_remote_copy(
            src_ref=edge2.at[0, n],
            dst_ref=halo2.at[0, n],
            send_sem=h2_send.at[0, n],
            recv_sem=h2_recv.at[0, n],
            device_id={"space": sp + 1},
            device_id_type=MESH,
        )

    def down2(n):
        return pltpu.make_async_remote_copy(
            src_ref=edge2.at[1, n],
            dst_ref=halo2.at[1, n],
            send_sem=h2_send.at[1, n],
            recv_sem=h2_recv.at[1, n],
            device_id={"space": sp - 1},
            device_id_type=MESH,
        )

    def project(act, w_ref, dst, buf, count, after):
        def body(n, carry):
            wide = pl.ds(pl.multiple_of(n * NCOL, NCOL), NCOL)
            y = jnp.dot(act[...], w_ref[:, wide], preferred_element_type=F32)
            dst[:, wide] = y
            s1 = fold(y)
            s2 = fold(y * y)
            for q in range(NCOL // LANES):
                part = slice(q * LANES, (q + 1) * LANES)
                put_stats(buf, sp, n * (NCOL // LANES) + q, count, s1[:, part], s2[:, part])
            after(n, y)
            return carry

        lax.fori_loop(0, count * LANES // NCOL, body, 0)

    n_wide = c_mid // NCOL
    early = n_wide // 2

    def send_edges(n, y):
        edge2[0, n] = y[pixels - edge :].astype(BF16)
        edge2[1, n] = y[:edge].astype(BF16)

        @pl.when(jnp.logical_and(has_bot, n < early))
        def _():
            up2(n).start()

        @pl.when(jnp.logical_and(has_top, n < early))
        def _():
            down2(n).start()

    def send_late():
        def body(n, carry):
            @pl.when(has_bot)
            def _():
                up2(n).start()

            @pl.when(has_top)
            def _():
                down2(n).start()

            return carry

        lax.fori_loop(early, n_wide, body, 0)

    load_w1.wait()
    project(act1, w1_ref, second, sa1, n_mid, send_edges)
    reduce_stats(1, n_mid, 2 * n_in, send_late)

    def wait_edges(n, carry):
        @pl.when(has_top)
        def _():
            up2(n).wait_recv()

        @pl.when(has_bot)
        def _():
            down2(n).wait_recv()

        return carry

    @pl.when(jnp.logical_not(has_top))
    def _():
        halo2[0] = jnp.zeros(halo2.shape[1:], BF16)

    @pl.when(jnp.logical_not(has_bot))
    def _():
        halo2[1] = jnp.zeros(halo2.shape[1:], BF16)

    lax.fori_loop(0, n_wide, wait_edges, 0)

    def conv2(n, carry):
        for q in range(NCOL // LANES):
            j = n * (NCOL // LANES) + q
            lanes = lanes_of(j)
            part = slice(q * LANES, (q + 1) * LANES)
            for r in range(rows):
                v = normal(second[r * cols : (r + 1) * cols, lanes], j)
                xp[j, r + RATE, PAD : PAD + cols, :] = v.astype(F32)
            top = normal(halo2[0, n, :, part].astype(F32), j).astype(F32)
            top = jnp.where(has_top, top, 0.0)
            bot = normal(halo2[1, n, :, part].astype(F32), j).astype(F32)
            bot = jnp.where(has_bot, bot, 0.0)
            for r in range(RATE):
                xp[j, r, PAD : PAD + cols, :] = top[r * cols : (r + 1) * cols]
                xp[j, rows + RATE + r, PAD : PAD + cols, :] = bot[r * cols : (r + 1) * cols]
            s1, s2 = conv_rows(j, list(range(rows)), d2_ref, second, zero8, zero8)
            put_stats(sa2, sp, j, n_mid, s1, s2)
        return carry

    lax.fori_loop(0, n_wide, conv2, 0)
    reduce_stats(2, n_mid, 2 * n_in + 2 * n_mid)
    norm_to(second, act3, n_mid)

    load_w2.wait()
    project(act3, w2_ref, fourth, sa3, n_out, lambda n, y: None)
    reduce_stats(3, n_out, 2 * n_in + 4 * n_mid)

    for q, ref in enumerate((mean_out, fac_out, shift_out)):
        for j in range(n_out):
            ref[0:1, j * LANES : (j + 1) * LANES] = coef[q, j : j + 1, :]

    def drain(n, carry):
        @pl.when(has_bot)
        def _():
            up2(n).wait_send()

        @pl.when(has_top)
        def _():
            down2(n).wait_send()

        return carry

    lax.fori_loop(0, n_wide, drain, 0)


def per_device(
    features,
    depth_one,
    gain_one,
    shift_one,
    point_one,
    gain_two,
    shift_two,
    depth_two,
    gain_three,
    shift_three,
    point_two,
    gain_four,
    shift_four,
):
    samples, span_rows, cols, c_in = features.shape
    rows = samples * span_rows
    assert samples == 1
    c_mid = point_one.shape[1]
    c_out = point_two.shape[1]
    pixels = rows * cols
    n_space = lax.axis_size("space")
    n_batch = lax.axis_size("batch")
    n_in, n_mid, n_out = c_in // LANES, c_mid // LANES, c_out // LANES
    any_spec = pl.BlockSpec(memory_space=pl.ANY)
    vmem = pl.BlockSpec(memory_space=pltpu.VMEM)
    counts = (n_in, n_mid, n_mid, n_out)
    edge = RATE * cols
    n_wide = c_mid // NCOL
    coef_rows = max(n_out, 8 * n_in)
    DMA = pltpu.SemaphoreType.DMA
    fourth, mean, fac, shift = pl.pallas_call(
        functools.partial(kernel, n_space, n_batch),
        out_shape=(
            pltpu.VMEM((pixels, c_out), F32),
            jax.ShapeDtypeStruct((1, c_out), F32),
            jax.ShapeDtypeStruct((1, c_out), F32),
            jax.ShapeDtypeStruct((1, c_out), F32),
        ),
        in_specs=[any_spec] * 3 + [vmem] * 10,
        out_specs=(vmem,) * 4,
        scratch_shapes=[
            pltpu.VMEM((rows, cols, c_in), BF16),
            pltpu.VMEM((c_in, c_mid), BF16),
            pltpu.VMEM((c_mid, c_out), BF16),
            pltpu.VMEM((2, RATE, cols, c_in), BF16),
            pltpu.VMEM((2, n_wide, edge, NCOL), BF16),
            pltpu.VMEM((2, n_wide, edge, NCOL), BF16),
            pltpu.VMEM((n_mid, rows + 2 * RATE, cols + 2 * PAD, LANES), F32),
            pltpu.VMEM((pixels, c_in), F32),
            pltpu.VMEM((pixels, c_in), BF16),
            pltpu.VMEM((pixels, c_mid), F32),
            pltpu.VMEM((pixels, c_mid), BF16),
            pltpu.VMEM((2 * sum((n_in, n_mid, n_mid, n_out)), LANES), F32),
        ]
        + [pltpu.VMEM((n_space, 2 * c, LANES), F32) for c in counts]
        + [pltpu.VMEM((n_batch, 2 * c, LANES), F32) for c in counts]
        + [
            pltpu.VMEM((5, coef_rows, LANES), F32),
            DMA((3,)),
            DMA((2, PIECES)),
            DMA((2, PIECES)),
            DMA((2, n_wide)),
            DMA((2, n_wide)),
            DMA((4, n_space - 1)),
            DMA((4, n_space - 1)),
            DMA((4, n_batch - 1)),
            DMA((4, n_batch - 1)),
        ],
        compiler_params=pltpu.CompilerParams(
            collective_id=0, has_side_effects=True, vmem_limit_bytes=56 * 1024 * 1024
        ),
        name="exit_block",
    )(
        features.reshape(rows, cols, c_in),
        point_one,
        point_two,
        depth_one,
        depth_two,
        *(
            v
            for v in (
                gain_one,
                shift_one,
                gain_two,
                shift_two,
                gain_three,
                shift_three,
                gain_four,
                shift_four,
            )
        ),
    )
    out = jnp.maximum((fourth - mean) * fac + shift, 0.0).astype(BF16)
    return out.reshape(samples, span_rows, cols, c_out)


def solution(mesh):
    return jax.shard_map(
        per_device,
        mesh=mesh,
        in_specs=(P("batch", "space", None, None),) + (P(),) * 12,
        out_specs=P("batch", "space", None, None),
        check_vma=False,
    )
```

```python
import functools

import jax
import jax.numpy as jnp
from jax import lax
from jax.experimental import pallas as pl
from jax.experimental.pallas import tpu as pltpu
from jax.sharding import PartitionSpec as P

RATE = 2
PIECES = 4
EPS = 1e-05
LANES = 128
PAD = 8
NCOL = 256
MESH = pl.DeviceIdType.MESH
F32 = jnp.float32
BF16 = jnp.bfloat16


def block_rows(pixels):
    for rows in (144, 96, 48, 32, 16):
        if pixels % rows == 0:
            return rows
    return pixels


def kernel(
    n_space,
    n_batch,
    x_hbm,
    w1_hbm,
    w2_hbm,
    d1_ref,
    d2_ref,
    g1_ref,
    b1_ref,
    g2_ref,
    b2_ref,
    g3_ref,
    b3_ref,
    g4_ref,
    b4_ref,
    fourth,
    mean_out,
    fac_out,
    shift_out,
    x_ref,
    w1_ref,
    w2_ref,
    halo1,
    edge2,
    halo2,
    xp,
    first,
    act1,
    second,
    act3,
    par_ref,
    sa0,
    sa1,
    sa2,
    sa3,
    sa4,
    sa5,
    sa6,
    sb0,
    sb1,
    sb2,
    sb3,
    sb4,
    sb5,
    sb6,
    coef,
    load_sem,
    h1_send,
    h1_recv,
    h2_send,
    h2_recv,
    a_send,
    a_recv,
    b_send,
    b_recv,
):
    rows, cols, c_in = x_hbm.shape
    c_mid = w1_hbm.shape[1]
    c_out = w2_hbm.shape[1]
    pixels = rows * cols
    edge = RATE * cols
    total = float(pixels * n_space * n_batch)
    step = block_rows(pixels)
    n_in, n_mid, n_out = c_in // LANES, c_mid // LANES, c_out // LANES
    sp = lax.axis_index("space")
    bt = lax.axis_index("batch")
    has_top = sp > 0
    has_bot = sp < n_space - 1
    sa = (sa0, sa1, sa2, sa3, sa4, sa5, sa6)
    sb = (sb0, sb1, sb2, sb3, sb4, sb5, sb6)

    load_x = pltpu.make_async_copy(x_hbm, x_ref, load_sem.at[0])
    load_w1 = pltpu.make_async_copy(w1_hbm, w1_ref, load_sem.at[1])
    load_w2 = pltpu.make_async_copy(w2_hbm, w2_ref, load_sem.at[2])

    barrier = pltpu.get_barrier_semaphore()
    for d in range(1, n_space):
        pl.semaphore_signal(
            barrier, inc=1, device_id={"space": lax.rem(sp + d, n_space)}, device_id_type=MESH
        )
    for d in range(1, n_batch):
        pl.semaphore_signal(
            barrier, inc=1, device_id={"batch": lax.rem(bt + d, n_batch)}, device_id_type=MESH
        )
    load_x.start()
    load_w1.start()
    load_w2.start()

    def clear(j, carry):
        for r in range(rows + 2 * RATE):
            xp[j, r, 0:PAD, :] = jnp.zeros((PAD, LANES), F32)
            xp[j, r, PAD + cols : PAD + cols + PAD, :] = jnp.zeros((PAD, LANES), F32)
        return carry

    lax.fori_loop(0, c_mid // LANES, clear, 0)
    at = 0
    for ref in (g1_ref, b1_ref, g2_ref, b2_ref, g3_ref, b3_ref, g4_ref, b4_ref):
        for j in range(ref.shape[0] // LANES):
            par_ref[at : at + 1, :] = ref[j * LANES : (j + 1) * LANES].reshape(1, LANES)
            at += 1
    load_x.wait()
    pl.semaphore_wait(barrier, n_space - 1 + n_batch - 1)

    wide_in = c_in // PIECES

    def up1(p):
        lanes = pl.ds(p * wide_in, wide_in)
        return pltpu.make_async_remote_copy(
            src_ref=x_ref.at[pl.ds(rows - RATE, RATE), :, lanes],
            dst_ref=halo1.at[0, :, :, lanes],
            send_sem=h1_send.at[0, p],
            recv_sem=h1_recv.at[0, p],
            device_id={"space": sp + 1},
            device_id_type=MESH,
        )

    def down1(p):
        lanes = pl.ds(p * wide_in, wide_in)
        return pltpu.make_async_remote_copy(
            src_ref=x_ref.at[pl.ds(0, RATE), :, lanes],
            dst_ref=halo1.at[1, :, :, lanes],
            send_sem=h1_send.at[1, p],
            recv_sem=h1_recv.at[1, p],
            device_id={"space": sp - 1},
            device_id_type=MESH,
        )

    for p in range(PIECES):

        @pl.when(has_bot)
        def _():
            up1(p).start()

        @pl.when(has_top)
        def _():
            down1(p).start()

    @pl.when(jnp.logical_not(has_top))
    def _():
        halo1[0] = jnp.zeros(halo1.shape[1:], BF16)

    @pl.when(jnp.logical_not(has_bot))
    def _():
        halo1[1] = jnp.zeros(halo1.shape[1:], BF16)

    def taps(d_ref, lanes):
        return [
            [d_ref[a, b : b + 1, lanes].astype(F32) for b in range(3)] for a in range(3)
        ]

    def conv_row(j, r, filt):
        acc = None
        for a in range(3):
            for b in range(3):
                term = xp[j, r + RATE * a, pl.ds(PAD + RATE * (b - 1), cols), :] * filt[a][b]
                acc = term if acc is None else acc + term
        return acc

    def lanes_of(j):
        return pl.ds(pl.multiple_of(j * LANES, LANES), LANES)

    def fold(v):
        s = v[0:8]
        for k in range(1, v.shape[0] // 8):
            s = s + v[8 * k : 8 * k + 8]
        return s

    def conv_rows(j, row_list, d_ref, dst, s1, s2):
        lanes = lanes_of(j)
        filt = taps(d_ref, lanes)
        for r in row_list:
            y = conv_row(j, r, filt)
            dst[r * cols : (r + 1) * cols, lanes] = y
            s1 = s1 + fold(y)
            s2 = s2 + fold(y * y)
        return s1, s2

    def put_stats(buf, slot, row, count, s1, s2):
        buf[slot, pl.ds(row, 1), :] = jnp.sum(s1, axis=0, keepdims=True)
        buf[slot, pl.ds(row + count, 1), :] = jnp.sum(s2, axis=0, keepdims=True)

    def exchange_a(i, d):
        return pltpu.make_async_remote_copy(
            src_ref=sa[i].at[sp],
            dst_ref=sa[i].at[sp],
            send_sem=a_send.at[i, d - 1],
            recv_sem=a_recv.at[i, d - 1],
            device_id={"space": lax.rem(sp + d, n_space)},
            device_id_type=MESH,
        )

    def exchange_b(i, d):
        return pltpu.make_async_remote_copy(
            src_ref=sb[i].at[bt],
            dst_ref=sb[i].at[bt],
            send_sem=b_send.at[i, d - 1],
            recv_sem=b_recv.at[i, d - 1],
            device_id={"batch": lax.rem(bt + d, n_batch)},
            device_id_type=MESH,
        )

    def start(i):
        for d in range(1, n_space):
            exchange_a(i, d).start()

    def relay(i):
        for d in range(1, n_space):
            exchange_a(i, d).wait_recv()
        s = sa[i][0]
        for k in range(1, n_space):
            s = s + sa[i][k]
        sb[i][bt] = s
        for d in range(1, n_batch):
            exchange_b(i, d).start()

    def finish(i, j0, count, at, full):
        for d in range(1, n_batch):
            exchange_b(i, d).wait_recv()
        s = sb[i][0]
        for k in range(1, n_batch):
            s = s + sb[i][k]
        mean = s[:count] / total
        var = s[count:] / total - mean * mean
        fac = par_ref[at + j0 : at + j0 + count] * lax.rsqrt(var + EPS)
        coef[0, j0 : j0 + count] = mean
        coef[1, j0 : j0 + count] = fac
        coef[2, j0 : j0 + count] = par_ref[at + full + j0 : at + full + j0 + count]
        for d in range(1, n_space):
            exchange_a(i, d).wait_send()
        for d in range(1, n_batch):
            exchange_b(i, d).wait_send()

    def normal(v, j):
        return jnp.maximum(
            (v - coef[0, pl.ds(j, 1), :]) * coef[1, pl.ds(j, 1), :] + coef[2, pl.ds(j, 1), :], 0.0
        ).astype(BF16)

    zero8 = jnp.zeros((8, LANES), F32)
    inner = list(range(RATE, rows - RATE))
    outer = list(range(RATE)) + list(range(rows - RATE, rows))


    def conv1_inner(j, carry):
        lanes = lanes_of(j)
        for r in range(rows):
            xp[j, r + RATE, PAD : PAD + cols, :] = x_ref[r, :, lanes].astype(F32)
        s1, s2 = conv_rows(j, inner, d1_ref, first, zero8, zero8)
        coef[3, pl.ds(pl.multiple_of(j * 8, 8), 8), :] = s1
        coef[4, pl.ds(pl.multiple_of(j * 8, 8), 8), :] = s2
        return carry

    lax.fori_loop(0, n_in, conv1_inner, 0)

    half_in = n_in // 2

    def conv1_outer(buf, j0):
        def body(j, carry):
            lanes = lanes_of(j)
            for r in range(RATE):
                xp[j, r, PAD : PAD + cols, :] = halo1[0, r, :, lanes].astype(F32)
                xp[j, rows + RATE + r, PAD : PAD + cols, :] = halo1[1, r, :, lanes].astype(F32)
            s1 = coef[3, pl.ds(pl.multiple_of(j * 8, 8), 8), :]
            s2 = coef[4, pl.ds(pl.multiple_of(j * 8, 8), 8), :]
            s1, s2 = conv_rows(j, outer, d1_ref, first, s1, s2)
            put_stats(buf, sp, j - j0, half_in, s1, s2)
            return carry

        return body

    for p in range(PIECES):

        @pl.when(has_top)
        def _():
            up1(p).wait_recv()

        @pl.when(has_bot)
        def _():
            down1(p).wait_recv()

        g = 2 * p // PIECES
        body = conv1_outer(sa[g], g * half_in)
        lax.fori_loop(p * n_in // PIECES, (p + 1) * n_in // PIECES, body, 0)
        if 2 * (p + 1) % PIECES == 0:
            start(g)

    relay(0)
    relay(1)
    finish(0, 0, half_in, 0, n_in)

    for p in range(PIECES):

        @pl.when(has_bot)
        def _():
            up1(p).wait_send()

        @pl.when(has_top)
        def _():
            down1(p).wait_send()

    def norm_to(src, dst, j0, j1):
        def body(j, carry):
            lanes = lanes_of(j)
            for k in range(pixels // step):
                span = slice(k * step, (k + 1) * step)
                dst[span, lanes] = normal(src[span, lanes], j)
            return carry

        lax.fori_loop(j0, j1, body, 0)

    def up2(n):
        return pltpu.make_async_remote_copy(
            src_ref=edge2.at[0, n],
            dst_ref=halo2.at[0, n],
            send_sem=h2_send.at[0, n],
            recv_sem=h2_recv.at[0, n],
            device_id={"space": sp + 1},
            device_id_type=MESH,
        )

    def down2(n):
        return pltpu.make_async_remote_copy(
            src_ref=edge2.at[1, n],
            dst_ref=halo2.at[1, n],
            send_sem=h2_send.at[1, n],
            recv_sem=h2_recv.at[1, n],
            device_id={"space": sp - 1},
            device_id_type=MESH,
        )

    per = NCOL // LANES

    def project_first(act, w_ref, dst, k1):
        def body(n, carry):
            wide = pl.ds(pl.multiple_of(n * NCOL, NCOL), NCOL)
            dst[:, wide] = jnp.dot(act[:, :k1], w_ref[:k1, wide], preferred_element_type=F32)
            return carry

        lax.fori_loop(0, dst.shape[1] // NCOL, body, 0)

    def project_rest(act, w_ref, dst, k0, n0, n1, buf, after):
        count = (n1 - n0) * per

        def body(n, carry):
            wide = pl.ds(pl.multiple_of(n * NCOL, NCOL), NCOL)
            y = jnp.dot(act[:, k0:], w_ref[k0:, wide], preferred_element_type=F32)
            y = y + dst[:, wide]
            dst[:, wide] = y
            s1 = fold(y)
            s2 = fold(y * y)
            for q in range(per):
                part = slice(q * LANES, (q + 1) * LANES)
                put_stats(buf, sp, (n - n0) * per + q, count, s1[:, part], s2[:, part])
            after(n, y)
            return carry

        lax.fori_loop(n0, n1, body, 0)

    n_wide = c_mid // NCOL
    early = n_wide // 2

    def send_edges(n, y):
        edge2[0, n] = y[pixels - edge :].astype(BF16)
        edge2[1, n] = y[:edge].astype(BF16)

        @pl.when(jnp.logical_and(has_bot, n < early))
        def _():
            up2(n).start()

        @pl.when(jnp.logical_and(has_top, n < early))
        def _():
            down2(n).start()

    def send_late():
        def body(n, carry):
            @pl.when(has_bot)
            def _():
                up2(n).start()

            @pl.when(has_top)
            def _():
                down2(n).start()

            return carry

        lax.fori_loop(early, n_wide, body, 0)

    half_mid = n_mid // 2
    norm_to(first, act1, 0, half_in)
    load_w1.wait()
    project_first(act1, w1_ref, second, half_in * LANES)
    finish(1, half_in, half_in, 0, n_in)
    norm_to(first, act1, half_in, n_in)
    project_rest(act1, w1_ref, second, half_in * LANES, 0, early, sa2, send_edges)
    start(2)
    project_rest(act1, w1_ref, second, half_in * LANES, early, n_wide, sa3, send_edges)
    start(3)
    send_late()
    relay(2)
    relay(3)

    def wait_edges(n, carry):
        @pl.when(has_top)
        def _():
            up2(n).wait_recv()

        @pl.when(has_bot)
        def _():
            down2(n).wait_recv()

        return carry

    @pl.when(jnp.logical_not(has_top))
    def _():
        halo2[0] = jnp.zeros(halo2.shape[1:], BF16)

    @pl.when(jnp.logical_not(has_bot))
    def _():
        halo2[1] = jnp.zeros(halo2.shape[1:], BF16)


    def conv2(buf, n0, n, carry):
        for q in range(NCOL // LANES):
            j = n * (NCOL // LANES) + q
            lanes = lanes_of(j)
            part = slice(q * LANES, (q + 1) * LANES)
            for r in range(rows):
                v = normal(second[r * cols : (r + 1) * cols, lanes], j)
                xp[j, r + RATE, PAD : PAD + cols, :] = v.astype(F32)
            top = normal(halo2[0, n, :, part].astype(F32), j).astype(F32)
            top = jnp.where(has_top, top, 0.0)
            bot = normal(halo2[1, n, :, part].astype(F32), j).astype(F32)
            bot = jnp.where(has_bot, bot, 0.0)
            for r in range(RATE):
                xp[j, r, PAD : PAD + cols, :] = top[r * cols : (r + 1) * cols]
                xp[j, rows + RATE + r, PAD : PAD + cols, :] = bot[r * cols : (r + 1) * cols]
            s1, s2 = conv_rows(j, list(range(rows)), d2_ref, second, zero8, zero8)
            put_stats(buf, sp, j - n0 * per, half_mid, s1, s2)
        return carry

    at2, at3 = 2 * n_in, 2 * n_in + 2 * n_mid
    finish(2, 0, half_mid, at2, n_mid)
    lax.fori_loop(0, early, wait_edges, 0)
    lax.fori_loop(0, early, functools.partial(conv2, sa4, 0), 0)
    start(4)
    finish(3, half_mid, half_mid, at2, n_mid)
    lax.fori_loop(early, n_wide, wait_edges, 0)
    lax.fori_loop(early, n_wide - 1, functools.partial(conv2, sa5, early), 0)
    relay(4)
    lax.fori_loop(n_wide - 1, n_wide, functools.partial(conv2, sa5, early), 0)
    start(5)
    finish(4, 0, half_mid, at3, n_mid)
    relay(5)

    norm_to(second, act3, 0, half_mid)
    load_w2.wait()
    project_first(act3, w2_ref, fourth, half_mid * LANES)
    finish(5, half_mid, half_mid, at3, n_mid)
    norm_to(second, act3, half_mid, n_mid)
    project_rest(act3, w2_ref, fourth, half_mid * LANES, 0, c_out // NCOL, sa6, lambda n, y: None)
    start(6)
    relay(6)
    finish(6, 0, n_out, 2 * n_in + 4 * n_mid, n_out)

    for q, ref in enumerate((mean_out, fac_out, shift_out)):
        for j in range(n_out):
            ref[0:1, j * LANES : (j + 1) * LANES] = coef[q, j : j + 1, :]

    def drain(n, carry):
        @pl.when(has_bot)
        def _():
            up2(n).wait_send()

        @pl.when(has_top)
        def _():
            down2(n).wait_send()

        return carry

    lax.fori_loop(0, n_wide, drain, 0)


def per_device(
    features,
    depth_one,
    gain_one,
    shift_one,
    point_one,
    gain_two,
    shift_two,
    depth_two,
    gain_three,
    shift_three,
    point_two,
    gain_four,
    shift_four,
):
    samples, span_rows, cols, c_in = features.shape
    rows = samples * span_rows
    assert samples == 1
    c_mid = point_one.shape[1]
    c_out = point_two.shape[1]
    pixels = rows * cols
    n_space = lax.axis_size("space")
    n_batch = lax.axis_size("batch")
    n_in, n_mid, n_out = c_in // LANES, c_mid // LANES, c_out // LANES
    any_spec = pl.BlockSpec(memory_space=pl.ANY)
    vmem = pl.BlockSpec(memory_space=pltpu.VMEM)
    counts = (n_in // 2,) * 2 + (n_mid // 2,) * 4 + (n_out,)
    edge = RATE * cols
    n_wide = c_mid // NCOL
    coef_rows = max(n_out, 8 * n_in)
    DMA = pltpu.SemaphoreType.DMA
    fourth, mean, fac, shift = pl.pallas_call(
        functools.partial(kernel, n_space, n_batch),
        out_shape=(
            pltpu.VMEM((pixels, c_out), F32),
            jax.ShapeDtypeStruct((1, c_out), F32),
            jax.ShapeDtypeStruct((1, c_out), F32),
            jax.ShapeDtypeStruct((1, c_out), F32),
        ),
        in_specs=[any_spec] * 3 + [vmem] * 10,
        out_specs=(vmem,) * 4,
        scratch_shapes=[
            pltpu.VMEM((rows, cols, c_in), BF16),
            pltpu.VMEM((c_in, c_mid), BF16),
            pltpu.VMEM((c_mid, c_out), BF16),
            pltpu.VMEM((2, RATE, cols, c_in), BF16),
            pltpu.VMEM((2, n_wide, edge, NCOL), BF16),
            pltpu.VMEM((2, n_wide, edge, NCOL), BF16),
            pltpu.VMEM((n_mid, rows + 2 * RATE, cols + 2 * PAD, LANES), F32),
            pltpu.VMEM((pixels, c_in), F32),
            pltpu.VMEM((pixels, c_in), BF16),
            pltpu.VMEM((pixels, c_mid), F32),
            pltpu.VMEM((pixels, c_mid), BF16),
            pltpu.VMEM((2 * sum((n_in, n_mid, n_mid, n_out)), LANES), F32),
        ]
        + [pltpu.VMEM((n_space, 2 * c, LANES), F32) for c in counts]
        + [pltpu.VMEM((n_batch, 2 * c, LANES), F32) for c in counts]
        + [
            pltpu.VMEM((5, coef_rows, LANES), F32),
            DMA((3,)),
            DMA((2, PIECES)),
            DMA((2, PIECES)),
            DMA((2, n_wide)),
            DMA((2, n_wide)),
            DMA((7, n_space - 1)),
            DMA((7, n_space - 1)),
            DMA((7, n_batch - 1)),
            DMA((7, n_batch - 1)),
        ],
        compiler_params=pltpu.CompilerParams(
            collective_id=0, has_side_effects=True, vmem_limit_bytes=56 * 1024 * 1024
        ),
        name="exit_block",
    )(
        features.reshape(rows, cols, c_in),
        point_one,
        point_two,
        depth_one,
        depth_two,
        *(
            v
            for v in (
                gain_one,
                shift_one,
                gain_two,
                shift_two,
                gain_three,
                shift_three,
                gain_four,
                shift_four,
            )
        ),
    )
    out = jnp.maximum((fourth - mean) * fac + shift, 0.0).astype(BF16)
    return out.reshape(samples, span_rows, cols, c_out)


def solution(mesh):
    return jax.shard_map(
        per_device,
        mesh=mesh,
        in_specs=(P("batch", "space", None, None),) + (P(),) * 12,
        out_specs=P("batch", "space", None, None),
        check_vma=False,
    )
```
